256 devices in a mesh: ens: 4 (over x), slab: 64 (over y, z, core).
Axes of the slice: x: 4, y: 4, z: 8, core: 2. Of those that a mesh axis runs over, the one named last changes fastest.
Arguments:
- velocity: float32 [4, 3, 8, 2048, 1024], P('ens', None, None, 'slab'), may hold values from -6 to 6
- cutoffs: int32 [4, 2, 8], P('ens'), may hold values from 128 to 511, as said below
- plane_index: int32 [4], P('ens'), may hold values from 0 to 2047
- boundary_index: int32 [4], P('ens'), may hold values from 0 to 2047
Outputs:
- blended: float32 [4, 3, 8, 2048, 1024], P('ens', None, None, 'slab')
The draws below stay inside these ranges and needn't reach their ends.
Inputs may be any that keep to these rules, and one draw needn't show every extreme that they name: `cutoffs`: row 0 lies in 256 to 511 and row 1 in 128 to 255; in every member some level has row 0 equal to 511 and some level has row 1 equal to 255.
All inputs are finite; a program needn't handle non-finite values.
Results may differ from the reference program's by a relative error of at most 0.0003.
Values sent between devices are 32-bit elements; how exact they have to be, the bound alone decides.
No kernel may reach another device: no remote copies, remote signals or barrier semaphores. Data moves between devices by JAX's collectives and lax.ppermute only.
A program may use at most 128 MiB of HBM per device.

```python
import jax
import jax.numpy as jnp
from jax import lax

NX = 2048
NY = 1024
KX = 512
KY = 256
COMP = 3
Z = 8
ENS = 4
N_ENS = 4


def draw_cutoffs(key, part):
    key_x, key_y, key_a, key_b = jax.random.split(jax.random.fold_in(key, 17), 4)
    levels = jnp.arange(Z, dtype=jnp.int32)
    cut_x = jax.random.randint(key_x, (N_ENS, Z), KX // 2, KX, dtype=jnp.int32)
    cut_y = jax.random.randint(key_y, (N_ENS, Z), KY // 2, KY, dtype=jnp.int32)
    top_x = jax.random.randint(key_a, (N_ENS, 1), 0, Z, dtype=jnp.int32)
    top_y = jax.random.randint(key_b, (N_ENS, 1), 0, Z, dtype=jnp.int32)
    cut_x = jnp.where(levels[None, :] == top_x, KX - 1, cut_x)
    cut_y = jnp.where(levels[None, :] == top_y, KY - 1, cut_y)
    return jnp.stack([cut_x, cut_y], axis=1).astype(jnp.int32)


def with_ends(values, rng, least, high):
    longest = values.shape.index(max(values.shape))
    spots = []
    for shift in (0, 1):
        where = [jax.random.randint(jax.random.fold_in(rng, axis), (), 0, length) for axis, length in enumerate(values.shape)]
        where[longest] = (where[longest] + shift) % values.shape[longest]
        spots.append(tuple(where))
    return values.at[spots[0]].set(least).at[spots[1]].set(high)


def level_of(stream_key, shape, cuts, low, high):
    gain, own = 1.0, jax.random.fold_in(stream_key, 6)
    for axis_at, blocks in cuts:
        steps = jnp.exp(jax.random.uniform(jax.random.fold_in(own, axis_at), (blocks,), jnp.float32, low / len(cuts), high / len(cuts)))
        gain = gain * jnp.repeat(steps, shape[axis_at] // blocks).reshape([-1 if axis == axis_at else 1 for axis in range(len(shape))])
    return gain


def bell_draw(stream_key, shape, deviation, bound, shards=(), kind=jnp.bfloat16):
    array = deviation * jax.random.normal(stream_key, shape, jnp.float32)
    if shards:
        array = array * level_of(stream_key, shape, shards, -0.22, 0.18)
    return jnp.clip(array, -bound, bound).astype(kind)


def setup_inputs(seed: int = 0) -> dict:
    splits = jax.random.split(jax.random.key(seed), 5)
    velocity = bell_draw(splits[0], (ENS, COMP, Z, NX, NY), 1.0, 6.0, ((0, 4), (3, 64)), jnp.float32)
    cutoffs = draw_cutoffs(jax.random.fold_in(splits[4], 71), 0)
    plane_index = with_ends(jax.random.randint(splits[2], (ENS,), 0, NX), jax.random.fold_in(splits[2], 1), 0, NX - 1).astype(jnp.int32)
    boundary_index = with_ends(jax.random.randint(splits[3], (ENS,), 0, NX), jax.random.fold_in(splits[3], 1), 0, NX - 1).astype(jnp.int32)
    return dict(velocity=velocity, cutoffs=cutoffs, plane_index=plane_index, boundary_index=boundary_index)


def filter_one(member_item):
    grid_values, cut_x, cut_y = member_item
    spectrum = jnp.fft.fft2(grid_values)
    wave_x = jnp.arange(NX, dtype=jnp.int32)
    wave_y = jnp.arange(NY, dtype=jnp.int32)
    kabs_x = jnp.minimum(wave_x, NX - wave_x)
    kabs_y = jnp.minimum(wave_y, NY - wave_y)
    keep = (kabs_x[:, None] <= cut_x) & (kabs_y[None, :] <= cut_y)
    kept = jnp.where(keep, spectrum, jnp.zeros_like(spectrum))
    return jnp.real(jnp.fft.ifft2(kept)).astype(grid_values.dtype)


def pick_plane(member_field, index_value):
    return lax.dynamic_index_in_dim(member_field, index_value.astype(jnp.int32), 2, keepdims=False)


def reference(velocity, cutoffs, plane_index, boundary_index):
    stacked = velocity.reshape(-1, NX, NY)
    cut_x = jnp.broadcast_to(cutoffs[:, 0][:, None, :], (N_ENS, COMP, Z)).reshape(-1)
    cut_y = jnp.broadcast_to(cutoffs[:, 1][:, None, :], (N_ENS, COMP, Z)).reshape(-1)
    filtered = lax.map(filter_one, (stacked, cut_x, cut_y)).reshape(velocity.shape)
    planes = jax.vmap(pick_plane)(filtered, plane_index)
    inflow = jnp.roll(planes, 1, axis=0)
    streamwise = jnp.arange(NX, dtype=jnp.int32)
    offset = jnp.abs(streamwise[None, :] - boundary_index.astype(jnp.int32)[:, None])
    distance = jnp.minimum(offset, NX - offset)
    relax = jnp.exp(-distance.astype(filtered.dtype) / (NX / 4.0))
    weight = relax[:, None, None, :, None]
    return filtered + weight * (inflow[:, :, :, None, :] - filtered)
```

```python
import functools
import math

import jax
import jax.numpy as jnp
import ml_dtypes
import numpy as np
from jax import lax
from jax.experimental import pallas as pl
from jax.experimental.pallas import tpu as pltpu
from jax.sharding import Mesh
from jax.sharding import PartitionSpec as P

NX = 2048
NY = 1024
KX = 512
KY = 256
COMP = 3
Z = 8
DEVICES = 64
ROWS = NX // DEVICES
SLAB = ("slab_0", "slab_1", "slab_2")

PIECE = (6, 8, 128)
LINES = 192
F32 = jnp.float32
BF16 = jnp.bfloat16
NN = (((1,), (0,)), ((), ()))
NT = (((1,), (1,)), ((), ()))


def halves(x):
    high = x.astype(BF16)
    return high, (x - high.astype(F32)).astype(BF16)


def dot3(left, right, dims):
    def one(a, b):
        return lax.dot_general(a, b, dims, preferred_element_type=F32)

    (lh, ll), (rh, rl) = left, right
    return one(lh, rh) + (one(ll, rh) + one(lh, rl))


def basis_y():
    row = np.arange(2 * KY)
    wave = 4 * (row // 8) + row % 4
    phase = (wave[:, None] * np.arange(NY)[None, :]) % NY
    angle = phase * (2.0 * np.pi / NY)
    table = np.where((row % 8 < 4)[:, None], np.cos(angle), np.sin(angle))
    high = table.astype(ml_dtypes.bfloat16)
    low = (table - high.astype(np.float64)).astype(ml_dtypes.bfloat16)
    return high, low


def basis_x():
    column = jnp.arange(2 * KX, dtype=jnp.int32)
    wave = 2 * (column % 256) + column // 512
    shift = jnp.where(column // 256 % 2 == 1, NX // 4, 0)
    place = jnp.arange(NX // 2, dtype=jnp.int32)
    phase = (place[:, None] * wave[None, :] - shift[None, :]) & (NX - 1)
    table = jnp.cos(phase.astype(F32) * (2.0 * math.pi / NX))
    high = lax.reduce_precision(table, 8, 7)
    return high.astype(BF16), (table - high).astype(BF16)


def analysis_kernel(cut_ref, v_ref, bh_ref, bl_ref, o_ref):
    field = v_ref[...].reshape(Z * ROWS, NY)
    spectra = dot3((bh_ref[...], bl_ref[...]), halves(field), NT)
    row = lax.broadcasted_iota(jnp.int32, spectra.shape, 0)
    level = lax.broadcasted_iota(jnp.int32, (1, Z * ROWS), 1) // ROWS
    cut = jnp.zeros((1, Z * ROWS), jnp.int32)
    for z in range(Z):
        cut = jnp.where(level == z, cut_ref[1, z], cut)
    wave = 4 * (row // 8) + row % 4
    weight = jnp.where(wave == 0, 1.0 / NY, 2.0 / NY)
    spectra = jnp.where(wave <= cut, spectra * weight, 0.0)
    for half in range(2):
        part = spectra[:, 128 * half : 128 * (half + 1)]
        o_ref[:, half] = part.reshape(DEVICES, 8, 128)


def swap_groups(rows):
    lane = lax.broadcasted_iota(jnp.int32, (1, 1, 128), 2)
    low = lane < 64
    even = lane // 32 % 2 == 0
    axis = rows[0].ndim - 1

    def roll(x, by):
        return pltpu.roll(x, by, axis)

    a, b, c, d = rows
    a, c = jnp.where(low, a, roll(c, 64)), jnp.where(low, roll(a, 64), c)
    b, d = jnp.where(low, b, roll(d, 64)), jnp.where(low, roll(b, 64), d)
    a, b = jnp.where(even, a, roll(b, 32)), jnp.where(even, roll(a, 96), b)
    c, d = jnp.where(even, c, roll(d, 32)), jnp.where(even, roll(c, 96), d)
    return a, b, c, d


def filter_kernel(cut_ref, plane_ref, r_ref, th_ref, tl_ref, o_ref, p_ref, fold_ref):
    half = DEVICES // 2
    for g in range(8):
        ahead = [r_ref[4 * g + i] for i in range(4)]
        behind = [r_ref[half + 4 * g + i] for i in range(4)]
        for parity in range(2):
            folded = [x - y if parity else x + y for x, y in zip(ahead, behind)]
            for i, rows in enumerate(swap_groups(folded)):
                fold_ref[parity, :, i, :, 128 * g : 128 * (g + 1)] = rows
    field = lax.broadcasted_iota(jnp.int32, (LINES, 1), 0) // 8
    cut = jnp.zeros((LINES, 1), jnp.int32)
    for z in range(Z):
        cut = jnp.where(field % Z == z, cut_ref[0, z], cut)
    column = lax.broadcasted_iota(jnp.int32, (1, KX), 1)
    parts = []
    for parity in range(2):
        columns = slice(KX * parity, KX * (parity + 1))
        table = (th_ref[:, columns], tl_ref[:, columns])
        lines = fold_ref[parity].reshape(LINES, NX // 2)
        coeffs = dot3(halves(lines), table, NN)
        wave = 2 * (column % 256) + parity
        weight = jnp.where(wave == 0, 1.0 / NX, 2.0 / NX)
        coeffs = jnp.where(wave <= cut, coeffs * weight, 0.0)
        parts.append(dot3(halves(coeffs), table, NT))
    ahead, behind = parts[0] + parts[1], parts[0] - parts[1]
    o_ref[0] = ahead
    o_ref[1] = behind
    place = lax.broadcasted_iota(jnp.int32, (1, NX // 2), 1)
    at = plane_ref[0]
    picked = jnp.where(place == at, ahead, 0.0) + jnp.where(place + NX // 2 == at, behind, 0.0)
    picked = jnp.sum(picked, axis=1, keepdims=True)
    lane = lax.broadcasted_iota(jnp.int32, (8, 128), 1)
    plane = jnp.zeros((8, 128), F32)
    for f in range(COMP * Z):
        plane = jnp.where(lane == f, picked[8 * f : 8 * (f + 1)], plane)
    p_ref[...] = plane


def blend_kernel(bound_ref, s_ref, p_ref, o_ref):
    plane = p_ref[...]
    lane = lax.broadcasted_iota(jnp.int32, (1, 1, 128), 2)
    for part in range(2):
        for g in range(8):
            place = lane + (NX // 2 * part + 128 * g)
            offset = jnp.abs(place - bound_ref[0])
            distance = jnp.minimum(offset, NX - offset)
            relax = jnp.exp(-distance.astype(F32) / (NX / 4.0))
            for t in range(6):
                mixed = []
                for i in range(4):
                    f = 4 * t + i
                    smooth = s_ref[part, 8 * f : 8 * (f + 1), 128 * g : 128 * (g + 1)]
                    inflow = plane[:, f : f + 1]
                    mixed.append((smooth + relax[0] * (inflow - smooth))[None])
                for i, rows in enumerate(swap_groups(mixed)):
                    o_ref[32 * part + 4 * g + i, t] = rows[0]


def synthesis_kernel(q_ref, bh_ref, bl_ref, o_ref):
    coeffs = jnp.concatenate([q_ref[:, h].reshape(2 * KY, 128).T for h in range(2)], axis=0)
    field = dot3(halves(coeffs), (bh_ref[...], bl_ref[...]), NN)
    o_ref[...] = field.reshape(Z, ROWS, NY)


VMEM = pltpu.MemorySpace.VMEM
SMEM = pltpu.MemorySpace.SMEM


def whole(space):
    return pl.BlockSpec(memory_space=space)


def params(**more):
    return pltpu.CompilerParams(vmem_limit_bytes=40 * 1024 * 1024, **more)


def on_device(velocity, cutoffs, plane_index, boundary_index):
    high, low = (jnp.asarray(table) for table in basis_y())
    cuts = cutoffs[0]
    table_spec = pl.BlockSpec((2 * KY, NY), lambda c: (0, 0))
    piece_spec = pl.BlockSpec((DEVICES, 2, 8, 128), lambda c: (0, c, 0, 0))
    field_spec = pl.BlockSpec((Z, ROWS, NY), lambda c: (c, 0, 0))
    spectra = pl.pallas_call(
        analysis_kernel,
        grid=(COMP,),
        in_specs=[whole(SMEM), field_spec, table_spec, table_spec],
        out_specs=piece_spec,
        out_shape=jax.ShapeDtypeStruct((DEVICES, *PIECE), F32),
        compiler_params=params(),
        name="analysis",
    )(cuts, velocity.reshape(COMP * Z, ROWS, NY), high, low)
    columns = lax.all_to_all(spectra, SLAB, 0, 0, tiled=True)
    smooth, plane = pl.pallas_call(
        filter_kernel,
        in_specs=[whole(SMEM), whole(SMEM), whole(VMEM), whole(VMEM), whole(VMEM)],
        out_specs=[whole(VMEM), whole(VMEM)],
        out_shape=[
            jax.ShapeDtypeStruct((2, LINES, NX // 2), F32),
            jax.ShapeDtypeStruct((8, 128), F32),
        ],
        scratch_shapes=[pltpu.VMEM((2, 6, 4, 8, NX // 2), F32)],
        compiler_params=params(),
        name="filter",
    )(cuts, plane_index, columns, *basis_x())
    members = lax.axis_size("ens")
    route = [((i - 1) % members, i) for i in range(members)]
    inflow = lax.ppermute(plane, "ens", route)
    blended = pl.pallas_call(
        blend_kernel,
        in_specs=[whole(SMEM), whole(VMEM), whole(VMEM)],
        out_specs=whole(VMEM),
        out_shape=jax.ShapeDtypeStruct((DEVICES, *PIECE), F32),
        compiler_params=params(),
        name="blend",
    )(boundary_index, smooth, inflow)
    returned = lax.all_to_all(blended, SLAB, 0, 0, tiled=True)
    result = pl.pallas_call(
        synthesis_kernel,
        grid=(COMP,),
        in_specs=[piece_spec, table_spec, table_spec],
        out_specs=field_spec,
        out_shape=jax.ShapeDtypeStruct((COMP * Z, ROWS, NY), F32),
        compiler_params=params(),
        name="synthesis",
    )(returned, high, low)
    return result.reshape(1, COMP, Z, ROWS, NY)


def solution(mesh):
    split = Mesh(
        mesh.devices.reshape(mesh.shape["ens"], 4, 8, 2), ("ens", "slab_0", "slab_1", "slab_2")
    )
    in_specs = (P("ens", None, None, SLAB, None), P("ens", None, None), P("ens"), P("ens"))
    out_specs = P("ens", None, None, SLAB, None)
    return jax.shard_map(
        on_device, mesh=split, in_specs=in_specs, out_specs=out_specs, check_vma=False
    )
```

```python
import jax
import jax.numpy as jnp
import ml_dtypes
import numpy as np
from jax import lax
from jax.experimental import pallas as pl
from jax.experimental.pallas import tpu as pltpu
from jax.sharding import Mesh
from jax.sharding import PartitionSpec as P

NX = 2048
NY = 1024
KX = 512
KY = 256
COMP = 3
Z = 8
DEVICES = 64
ROWS = NX // DEVICES
SLAB = ("slab_0", "slab_1", "slab_2")

PIECE = (6, 8, 128)
QUARTER = NX // 4
READY = (0, 20, 42, 64)
F32 = jnp.float32
BF16 = jnp.bfloat16
VMEM = pltpu.MemorySpace.VMEM
SMEM = pltpu.MemorySpace.SMEM
HBM = pltpu.MemorySpace.HBM


def halves(x):
    high = x.astype(BF16)
    return high, (x - high.astype(F32)).astype(BF16)


def dot3(left, right):
    def one(a, b):
        return jnp.dot(a, b, preferred_element_type=F32)

    (lh, ll), (rh, rl) = left, right
    return one(lh, rh) + (one(ll, rh) + one(lh, rl))


def basis_y():
    parity = np.arange(2)[:, None, None]
    place = np.arange(NY // 2)[None, :, None]
    column = np.arange(KY)[None, None, :]
    phase = (place * (2 * (column % 128) + parity)) % NY
    angle = phase * (2.0 * np.pi / NY)
    table = np.where(column < 128, np.cos(angle), np.sin(angle))
    high = table.astype(ml_dtypes.bfloat16)
    low = (table - high.astype(np.float64)).astype(ml_dtypes.bfloat16)
    return np.stack([high, low], axis=1)


GROUPS = (0, 2, 1, 3)


def turns(left, right):
    phase = (left * right) % NX
    angle = phase * (2.0 * np.pi / NX)
    return np.stack([np.cos(angle), np.sin(angle)]).astype(np.float32)


def angle_parts():
    place = np.arange(QUARTER)[None, :]
    sixteen = np.arange(16)[:, None]
    coarse = turns(64 * np.arange(8)[:, None], place)
    fine = np.stack([turns(4 * sixteen + g, place) for g in GROUPS])
    wave = 4 * np.arange(128)[None, :]
    far = np.stack([turns(wave + g, 16 * np.arange(32)[:, None]) for g in GROUPS])
    near = np.stack([turns(wave + g, sixteen) for g in GROUPS])
    return coarse, fine, far, near


def products(a, b):
    return a[0] * b[0] - a[1] * b[1], a[1] * b[0] + a[0] * b[1]


def store(high_ref, low_ref, rows, columns, value):
    high_ref[rows, columns], low_ref[rows, columns] = halves(value)


def rows_of_waves(n_ref, ca_ref, fi_ref, fh_ref, fl_ref, t_ref):
    at = n_ref[1]
    plane = lax.broadcasted_iota(jnp.int32, (16, QUARTER), 1) == at % QUARTER

    def picked(value):
        return jnp.sum(jnp.where(plane, value, 0.0), axis=1, keepdims=True)

    for g in range(4):
        fine = fi_ref[g, 0], fi_ref[g, 1]
        turn = at // QUARTER * GROUPS[g] % 4
        cosine = jnp.where(turn % 2 == 0, 1 - turn, 0).astype(F32)
        sine = jnp.where(turn % 2 == 1, 2 - turn, 0).astype(F32)
        for n in range(8):
            coarse = ca_ref[0, n : n + 1], ca_ref[1, n : n + 1]
            first = 256 * g + 16 * n
            pair = products(coarse, fine)
            for i in range(2):
                rows = slice(first + 128 * i, first + 128 * i + 16)
                store(fh_ref, fl_ref, rows, slice(None), pair[i])
            c, s = picked(pair[0]), picked(pair[1])
            t_ref[first : first + 16] = jnp.broadcast_to(cosine * c - sine * s, (16, 128))
            t_ref[first + 128 : first + 144] = jnp.broadcast_to(sine * c + cosine * s, (16, 128))


def rows_of_places(fa_ref, ne_ref, ih_ref, il_ref):
    for g in range(4):
        near = ne_ref[g, 0], ne_ref[g, 1]
        for b in range(32):
            far = fa_ref[g, 0, b : b + 1], fa_ref[g, 1, b : b + 1]
            for i, value in enumerate(products(far, near)):
                first = 256 * g + 128 * i
                store(ih_ref, il_ref, slice(16 * b, 16 * b + 16), slice(first, first + 128), value)


def weights(n_ref, w_ref):
    def relax(place):
        offset = jnp.abs(place - n_ref[2])
        distance = jnp.minimum(offset, NX - offset)
        return jnp.exp(-distance.astype(F32) / (NX / 4.0))

    for g in range(8):
        place = 32 * (8 * g + lax.broadcasted_iota(jnp.int32, (8, 4, 8, 128), 0))
        place += 8 * lax.broadcasted_iota(jnp.int32, place.shape, 1)
        place += lax.broadcasted_iota(jnp.int32, place.shape, 2)
        w_ref[8 * g : 8 * g + 8, 0:4] = relax(place)
        rest = place[:, 0:2]
        w_ref[8 * g : 8 * g + 8, 4:6] = relax(jnp.where(half_lanes(rest), rest, rest + 16))


def half_lanes(x):
    return lax.broadcasted_iota(jnp.int32, (1,) * (x.ndim - 1) + (128,), x.ndim - 1) < 64


def swapped(x):
    return pltpu.roll(x, 64, x.ndim - 1)


def analysis_kernel(v_hbm, cut_hbm, table_hbm, o_hbm, o_ref, v_ref, cut_ref, table_ref, sems):
    copies = [
        pltpu.make_async_copy(table_hbm, table_ref, sems.at[COMP]),
        pltpu.make_async_copy(cut_hbm, cut_ref, sems.at[COMP + 1]),
    ]
    for c in range(COMP):
        fields = pl.ds(Z * c, Z)
        copies.append(
            pltpu.make_async_copy(v_hbm.at[fields], v_ref.at[fields], sems.at[c])
        )
    for copy in copies:
        copy.start()
    for copy in copies[:2]:
        copy.wait()
    lane = lax.broadcasted_iota(jnp.int32, (1, KY), 1) % 128
    for c in range(COMP):
        copies[2 + c].wait()
        field = v_ref[Z * c : Z * (c + 1)].reshape(Z * ROWS, NY)
        left, right = field[:, : NY // 2], field[:, NY // 2 :]
        for parity in range(2):
            folded = left - right if parity else left + right
            spectra = dot3(halves(folded), (table_ref[parity, 0], table_ref[parity, 1]))
            wave = 2 * lane + parity
            weight = jnp.where(wave == 0, 1.0 / NY, 2.0 / NY)
            for z in range(Z):
                scale = jnp.where(wave <= cut_ref[0, 1, z], weight, 0.0)
                own = spectra[ROWS * z : ROWS * (z + 1)] * scale
                for part in range(2):
                    block = 4 * (Z * c + z) + 2 * parity + part
                    values = own[:, 128 * part : 128 * (part + 1)]
                    first = block // 3 * 2
                    if block % 3 != 1:
                        o_ref[first + block % 3 // 2, 0:4] = values.reshape(4, 8, 128)
                        continue
                    above, below = values[:16], values[16:]
                    low = half_lanes(above)
                    even = jnp.where(low, above, swapped(below))
                    odd = jnp.where(low, swapped(above), below)
                    o_ref[first, 4:6] = even.reshape(2, 8, 128)
                    o_ref[first + 1, 4:6] = odd.reshape(2, 8, 128)
        ready = slice(READY[c], READY[c + 1])
        copies.append(
            pltpu.make_async_copy(o_ref.at[ready], o_hbm.at[ready], sems.at[COMP + 2 + c])
        )
        copies[-1].start()
    for copy in copies[2 + COMP :]:
        copy.wait()


def forward_kernel(n_ref, r_ref, ca_ref, fi_ref, c_ref, p_ref, fh_ref, fl_ref, t_ref):
    rows_of_waves(n_ref, ca_ref, fi_ref, fh_ref, fl_ref, t_ref)
    quarters = []
    for u in range(4):
        owned = slice(16 * u, 16 * (u + 1))
        main = r_ref[owned, 0:4].reshape(QUARTER, 128)
        rest = r_ref[owned, 4:6]
        rest = jnp.concatenate([rest, swapped(rest)], axis=1).reshape(QUARTER, 128)
        quarters.append(jnp.concatenate([main, rest], axis=1))
    v0, v1, v2, v3 = quarters
    even, odd = v0 + v2, v1 + v3
    inputs = [halves(even + odd), halves(even - odd), halves(v0 - v2), halves(v1 - v3)]

    def ahead(rows, data):
        return dot3((fh_ref[rows], fl_ref[rows]), data)

    x0 = ahead(slice(0, 256), inputs[0])
    x2 = ahead(slice(256, 512), inputs[1])
    yc = ahead(slice(512, 1024), inputs[2])
    yd = ahead(slice(512, 1024), inputs[3])
    device = n_ref[0]
    pair = device // 2
    whole = (3 * pair + 2 * (device % 2)) // 4 % Z
    shared = (3 * pair + 1) // 4 % Z
    lane = lax.broadcasted_iota(jnp.int32, (1, 256), 1)
    cut = jnp.where(lane < 128, n_ref[3 + whole], n_ref[3 + shared])
    index = lax.broadcasted_iota(jnp.int32, (128, 1), 0)

    def kept(values, group):
        wave = 4 * index + group
        weight = jnp.where(wave == 0, 1.0 / NX, 2.0 / NX)
        return jnp.where(wave <= cut, values * weight, 0.0)

    def part(values, i):
        return values[128 * i : 128 * (i + 1)]

    re1 = kept(part(yc, 0) - part(yd, 1), 1)
    im1 = kept(part(yc, 1) + part(yd, 0), 1)
    re3 = kept(part(yc, 2) + part(yd, 3), 3)
    im3 = kept(part(yc, 3) - part(yd, 2), 3)

    coeffs = jnp.concatenate(
        [
            kept(part(x0, 0), 0),
            kept(part(x0, 1), 0),
            kept(part(x2, 0), 2),
            kept(part(x2, 1), 2),
            re1,
            im1,
            re3,
            im3,
        ],
        axis=0,
    )
    c_ref[0], c_ref[1] = halves(coeffs)
    column = t_ref[...]
    row = jnp.concatenate(
        [jnp.sum(column * coeffs[:, 128 * i : 128 * (i + 1)], axis=0, keepdims=True) for i in range(2)],
        axis=1,
    )
    p_ref[...] = jnp.broadcast_to(row, (8, 256))


def inverse_kernel(n_ref, c_ref, fa_ref, ne_ref, o_ref, w_ref, ih_ref, il_ref):
    rows_of_places(fa_ref, ne_ref, ih_ref, il_ref)
    weights(n_ref, w_ref)

    def back(columns, data):
        return dot3((ih_ref[:, columns], il_ref[:, columns]), data)

    def rows(i, first, last):
        return c_ref[i, 128 * first : 128 * last]

    p0 = back(slice(0, 256), (rows(0, 0, 2), rows(1, 0, 2)))
    p2 = back(slice(256, 512), (rows(0, 2, 4), rows(1, 2, 4)))
    co = back(slice(512, 1024), (rows(0, 4, 8), rows(1, 4, 8)))
    turned = [
        jnp.concatenate([rows(i, 5, 6), -rows(i, 4, 5), -rows(i, 7, 8), rows(i, 6, 7)], axis=0)
        for i in range(2)
    ]
    do = back(slice(512, 1024), turned)
    even, odd = p0 + p2, p0 - p2
    for u, value in enumerate((even + co, odd + do, even - co, odd - do)):
        owned = slice(16 * u, 16 * (u + 1))
        o_ref[owned, 0:4] = value[:, :128].reshape(16, 4, 8, 128)
        rest = value[:, 128:].reshape(16, 4, 8, 128)
        above, below = rest[:, 0:2], rest[:, 2:4]
        o_ref[owned, 4:6] = jnp.where(half_lanes(above), above, swapped(below))


def blend_kernel(s_ref, w_ref, p_ref, o_ref):
    whole = p_ref[0:1, :128]
    shared = p_ref[0:1, 128:]
    shared = jnp.where(half_lanes(shared), shared, swapped(shared))
    for tiles, inflow in ((slice(0, 4), whole), (slice(4, 6), shared)):
        smooth = s_ref[:, tiles]
        o_ref[:, tiles] = smooth + w_ref[:, tiles] * (inflow[None, None] - smooth)


def synthesis_kernel(q_ref, table_ref, o_hbm, o_ref, sems):
    copies = []
    for c in range(COMP):
        sums = []
        for parity in range(2):
            rows = []
            for z in range(Z):
                blocks = []
                for part in range(2):
                    block = 4 * (Z * c + z) + 2 * parity + part
                    first = block // 3 * 2
                    if block % 3 != 1:
                        blocks.append(q_ref[first + block % 3 // 2, 0:4].reshape(ROWS, 128))
                        continue
                    even = q_ref[first, 4:6].reshape(16, 128)
                    odd = q_ref[first + 1, 4:6].reshape(16, 128)
                    low = half_lanes(even)
                    above = jnp.where(low, even, swapped(odd))
                    below = jnp.where(low, swapped(even), odd)
                    blocks.append(jnp.concatenate([above, below], axis=0))
                rows.append(jnp.concatenate(blocks, axis=1))
            data = halves(jnp.concatenate(rows, axis=0))
            sums.append(dot3(data, (table_ref[parity, 0], table_ref[parity, 1])))
        fields = slice(Z * c, Z * (c + 1))
        o_ref[fields, :, : NY // 2] = (sums[0] + sums[1]).reshape(Z, ROWS, NY // 2)
        o_ref[fields, :, NY // 2 :] = (sums[0] - sums[1]).reshape(Z, ROWS, NY // 2)
        fields = pl.ds(Z * c, Z)
        copies.append(
            pltpu.make_async_copy(o_ref.at[fields], o_hbm.at[fields], sems.at[c])
        )
        copies[-1].start()
    for copy in copies:
        copy.wait()


def whole(space):
    return pl.BlockSpec(memory_space=space)


def params(mib):
    return pltpu.CompilerParams(vmem_limit_bytes=mib * 1024 * 1024)


def shape(*dims, kind=F32):
    return jax.ShapeDtypeStruct(dims, kind)


PIECES = shape(DEVICES, *PIECE)
FIELDS = (COMP * Z, ROWS, NY)


def on_device(velocity, cutoffs, plane_index, boundary_index):
    table_y = basis_y()
    spectra = pl.pallas_call(
        analysis_kernel,
        in_specs=[whole(HBM)] * 3,
        out_specs=whole(HBM),
        out_shape=PIECES,
        scratch_shapes=[
            pltpu.VMEM(PIECES.shape, F32),
            pltpu.VMEM(FIELDS, F32),
            pltpu.SMEM((1, 2, Z), jnp.int32),
            pltpu.VMEM((2, 2, NY // 2, KY), BF16),
            pltpu.SemaphoreType.DMA((2 * COMP + 2,)),
        ],
        compiler_params=params(63),
        name="analysis",
    )(velocity.reshape(FIELDS), cutoffs, jnp.asarray(table_y))
    columns = lax.all_to_all(spectra, SLAB, 0, 0, tiled=True)
    device = lax.axis_index(SLAB).astype(jnp.int32).reshape(1)
    numbers = jnp.concatenate([device, plane_index, boundary_index, cutoffs[0, 0]])
    coarse, fine, far, near = (jnp.asarray(part) for part in angle_parts())
    coeffs, plane = pl.pallas_call(
        forward_kernel,
        in_specs=[whole(SMEM)] + [whole(VMEM)] * 3,
        out_specs=[whole(VMEM)] * 2,
        out_shape=[shape(2, 2 * KX, 256, kind=BF16), shape(8, 256)],
        scratch_shapes=[pltpu.VMEM((2 * KX, QUARTER), BF16)] * 2 + [pltpu.VMEM((2 * KX, 128), F32)],
        compiler_params=params(24),
        name="forward",
    )(numbers, columns, coarse, fine)
    members = lax.axis_size("ens")
    route = [((i - 1) % members, i) for i in range(members)]
    inflow = lax.ppermute(plane, "ens", route)
    smooth, weight = pl.pallas_call(
        inverse_kernel,
        in_specs=[whole(SMEM)] + [whole(VMEM)] * 3,
        out_specs=[whole(VMEM)] * 2,
        out_shape=[PIECES] * 2,
        scratch_shapes=[pltpu.VMEM((QUARTER, 2 * KX), BF16)] * 2,
        compiler_params=params(24),
        cost_estimate=pl.CostEstimate(flops=1 << 30, bytes_accessed=1 << 22, transcendentals=0),
        name="inverse",
    )(numbers, coeffs, far, near)
    blended = pl.pallas_call(
        blend_kernel,
        in_specs=[whole(VMEM)] * 3,
        out_specs=whole(VMEM),
        out_shape=PIECES,
        compiler_params=params(8),
        name="blend",
    )(smooth, weight, inflow)
    returned = lax.all_to_all(blended, SLAB, 0, 0, tiled=True)
    result = pl.pallas_call(
        synthesis_kernel,
        in_specs=[whole(VMEM), whole(VMEM)],
        out_specs=whole(HBM),
        out_shape=shape(*FIELDS),
        scratch_shapes=[pltpu.VMEM(FIELDS, F32), pltpu.SemaphoreType.DMA((COMP,))],
        compiler_params=params(24),
        name="synthesis",
    )(returned, jnp.asarray(table_y.transpose(0, 1, 3, 2)))
    return result.reshape(1, COMP, Z, ROWS, NY)


def solution(mesh):
    split = Mesh(
        mesh.devices.reshape(mesh.shape["ens"], 4, 8, 2), ("ens", "slab_0", "slab_1", "slab_2")
    )
    in_specs = (P("ens", None, None, SLAB, None), P("ens", None, None), P("ens"), P("ens"))
    out_specs = P("ens", None, None, SLAB, None)
    return jax.shard_map(
        on_device, mesh=split, in_specs=in_specs, out_specs=out_specs, check_vma=False
    )
```

```python
import jax
import jax.numpy as jnp
import ml_dtypes
import numpy as np
from jax import lax
from jax.experimental import pallas as pl
from jax.experimental.pallas import tpu as pltpu
from jax.sharding import Mesh
from jax.sharding import PartitionSpec as P

NX = 2048
NY = 1024
KX = 512
KY = 256
COMP = 3
Z = 8
DEVICES = 64
ROWS = NX // DEVICES
SLAB = ("slab_0", "slab_1", "slab_2")

PIECE = (6, 8, 128)
QUARTER = NX // 4
CHUNKS = ((0, 8), (8, 16), (16, 20), (20, 24))
F32 = jnp.float32
BF16 = jnp.bfloat16
VMEM = pltpu.MemorySpace.VMEM
SMEM = pltpu.MemorySpace.SMEM
HBM = pltpu.MemorySpace.HBM


def halves(x):
    high = x.astype(BF16)
    return high, (x - high.astype(F32)).astype(BF16)


def dot3(left, right):
    def one(a, b):
        return jnp.dot(a, b, preferred_element_type=F32)

    (lh, ll), (rh, rl) = left, right
    return one(lh, rh) + (one(ll, rh) + one(lh, rl))


def basis_y():
    parity = np.arange(2)[:, None, None]
    row = np.arange(KY)[None, :, None]
    place = np.arange(NY // 2)[None, None, :]
    phase = (place * (2 * (row % 128) + parity)) % NY
    angle = phase * (2.0 * np.pi / NY)
    table = np.where(row < 128, np.cos(angle), np.sin(angle))
    high = table.astype(ml_dtypes.bfloat16)
    low = (table - high.astype(np.float64)).astype(ml_dtypes.bfloat16)
    return np.stack([high, low], axis=1)


def parts_y():
    wave = 2 * np.arange(128)[None, :]
    place = np.concatenate([16 * np.arange(32), np.arange(16)])[:, None]
    return np.stack([turns(wave + parity, place, NY) for parity in range(2)])


GROUPS = (0, 2, 1, 3)


def turns(left, right, length=NX):
    phase = (left * right) % length
    angle = phase * (2.0 * np.pi / length)
    return np.stack([np.cos(angle), np.sin(angle)]).astype(np.float32)


def angle_parts():
    place = np.arange(QUARTER)[None, :]
    sixteen = np.arange(16)[:, None]
    coarse = turns(64 * np.arange(8)[:, None], place)
    fine = np.stack([turns(4 * sixteen + g, place) for g in GROUPS])
    wave = 4 * np.arange(128)[None, :]
    far = np.stack([turns(wave + g, 16 * np.arange(32)[:, None]) for g in GROUPS])
    near = np.stack([turns(wave + g, sixteen) for g in GROUPS])
    return coarse, fine, far, near


def products(a, b):
    return a[0] * b[0] - a[1] * b[1], a[1] * b[0] + a[0] * b[1]


def store(high_ref, low_ref, rows, columns, value):
    high_ref[rows, columns], low_ref[rows, columns] = halves(value)


def rows_of_waves(plane_ref, ca_ref, fi_ref, fh_ref, fl_ref, t_ref):
    at = plane_ref[0]

    def picked(value):
        here = lax.broadcasted_iota(jnp.int32, value.shape, 1) == at % QUARTER
        return jnp.sum(jnp.where(here, value, 0.0), axis=1, keepdims=True)

    coarse_at = picked(ca_ref[0]), picked(ca_ref[1])
    for g in range(4):
        fine = fi_ref[g, 0], fi_ref[g, 1]
        turn = at // QUARTER * GROUPS[g] % 4
        cosine = jnp.where(turn % 2 == 0, 1 - turn, 0).astype(F32)
        sine = jnp.where(turn % 2 == 1, 2 - turn, 0).astype(F32)
        c, s = picked(fine[0]), picked(fine[1])
        fine_at = cosine * c - sine * s, sine * c + cosine * s
        for n in range(8):
            coarse = ca_ref[0, n : n + 1], ca_ref[1, n : n + 1]
            there = coarse_at[0][n : n + 1], coarse_at[1][n : n + 1]
            values, at_plane = products(coarse, fine), products(there, fine_at)
            for i in range(2):
                first = 256 * g + 128 * i + 16 * n
                rows = slice(first, first + 16)
                store(fh_ref, fl_ref, rows, slice(None), values[i])
                t_ref[rows] = jnp.broadcast_to(at_plane[i], (16, 128))


def rows_of_places(fa_ref, ne_ref, ih_ref, il_ref):
    for g in range(4):
        near = ne_ref[g, 0], ne_ref[g, 1]
        for b in range(32):
            far = fa_ref[g, 0, b : b + 1], fa_ref[g, 1, b : b + 1]
            for i, value in enumerate(products(far, near)):
                first = 256 * g + 128 * i
                store(ih_ref, il_ref, slice(16 * b, 16 * b + 16), slice(first, first + 128), value)


def weights(bound_ref, w_ref):
    def relax(place):
        offset = jnp.abs(place - bound_ref[0])
        distance = jnp.minimum(offset, NX - offset)
        return jnp.exp(-distance.astype(F32) / (NX / 4.0))

    for g in range(8):
        place = 32 * (8 * g + lax.broadcasted_iota(jnp.int32, (8, 4, 8, 128), 0))
        place += 8 * lax.broadcasted_iota(jnp.int32, place.shape, 1)
        place += lax.broadcasted_iota(jnp.int32, place.shape, 2)
        w_ref[8 * g : 8 * g + 8, 0:4] = relax(place)
        rest = place[:, 0:2]
        w_ref[8 * g : 8 * g + 8, 4:6] = relax(jnp.where(half_lanes(rest), rest, rest + 16))


def half_lanes(x):
    return lax.broadcasted_iota(jnp.int32, (1,) * (x.ndim - 1) + (128,), x.ndim - 1) < 64


def swapped(x):
    return pltpu.roll(x, 64, x.ndim - 1)


def analysis_kernel(
    v_hbm, cut_hbm, part_hbm, o_hbm, o_ref, v_ref, cut_ref, part_ref, table_ref, sems
):
    copies = [
        pltpu.make_async_copy(part_hbm, part_ref, sems.at[0]),
        pltpu.make_async_copy(cut_hbm, cut_ref, sems.at[1]),
    ]
    for i, (first, last) in enumerate(CHUNKS):
        fields = pl.ds(first, last - first)
        copies.append(
            pltpu.make_async_copy(v_hbm.at[fields], v_ref.at[fields], sems.at[2 + i])
        )
    for copy in copies:
        copy.start()
    for copy in copies[:2]:
        copy.wait()
    for parity in range(2):
        near = part_ref[parity, 0, 32:48], part_ref[parity, 1, 32:48]
        for b in range(32):
            far = part_ref[parity, 0, b : b + 1], part_ref[parity, 1, b : b + 1]
            for i, value in enumerate(products(far, near)):
                rows, columns = slice(16 * b, 16 * b + 16), slice(128 * i, 128 * i + 128)
                high, low = halves(value)
                table_ref[parity, 0, rows, columns] = high
                table_ref[parity, 1, rows, columns] = low
    lane = lax.broadcasted_iota(jnp.int32, (1, KY), 1) % 128
    sent = 0
    for i, (begin, end) in enumerate(CHUNKS):
        copies[2 + i].wait()
        field = v_ref[begin:end].reshape((end - begin) * ROWS, NY)
        left, right = field[:, : NY // 2], field[:, NY // 2 :]
        for parity in range(2):
            folded = left - right if parity else left + right
            spectra = dot3(halves(folded), (table_ref[parity, 0], table_ref[parity, 1]))
            wave = 2 * lane + parity
            weight = jnp.where(wave == 0, 1.0 / NY, 2.0 / NY)
            for f in range(begin, end):
                scale = jnp.where(wave <= cut_ref[0, 1, f % Z], weight, 0.0)
                own = spectra[ROWS * (f - begin) : ROWS * (f - begin + 1)] * scale
                for part in range(2):
                    block = 4 * f + 2 * parity + part
                    values = own[:, 128 * part : 128 * (part + 1)]
                    first = block // 3 * 2
                    if block % 3 != 1:
                        o_ref[first + block % 3 // 2, 0:4] = values.reshape(4, 8, 128)
                        continue
                    above, below = values[:16], values[16:]
                    low = half_lanes(above)
                    even = jnp.where(low, above, swapped(below))
                    odd = jnp.where(low, swapped(above), below)
                    o_ref[first, 4:6] = even.reshape(2, 8, 128)
                    o_ref[first + 1, 4:6] = odd.reshape(2, 8, 128)
        ready = pl.ds(sent, 4 * end // 3 * 2 - sent)
        sent = 4 * end // 3 * 2
        done = pltpu.make_async_copy(
            o_ref.at[ready], o_hbm.at[ready], sems.at[2 + len(CHUNKS) + i]
        )
        done.start()
        copies.append(done)
    for copy in copies[2 + len(CHUNKS) :]:
        copy.wait()


def forward_kernel(cut_ref, plane_ref, r_ref, ca_ref, fi_ref, c_ref, p_ref, fh_ref, fl_ref, t_ref):
    rows_of_waves(plane_ref, ca_ref, fi_ref, fh_ref, fl_ref, t_ref)
    quarters = []
    for u in range(4):
        owned = slice(16 * u, 16 * (u + 1))
        main = r_ref[owned, 0:4].reshape(QUARTER, 128)
        rest = r_ref[owned, 4:6]
        rest = jnp.concatenate([rest, swapped(rest)], axis=1).reshape(QUARTER, 128)
        quarters.append(jnp.concatenate([main, rest], axis=1))
    v0, v1, v2, v3 = quarters
    even, odd = v0 + v2, v1 + v3
    inputs = [halves(even + odd), halves(even - odd), halves(v0 - v2), halves(v1 - v3)]

    def ahead(rows, data):
        return dot3((fh_ref[rows], fl_ref[rows]), data)

    x0 = ahead(slice(0, 256), inputs[0])
    x2 = ahead(slice(256, 512), inputs[1])
    yc = ahead(slice(512, 1024), inputs[2])
    yd = ahead(slice(512, 1024), inputs[3])
    pair = 8 * lax.axis_index("slab_0") + lax.axis_index("slab_1")
    whole = (3 * pair + 2 * lax.axis_index("slab_2")) // 4 % Z
    shared = (3 * pair + 1) // 4 % Z
    lane = lax.broadcasted_iota(jnp.int32, (1, 256), 1)
    cuts = cut_ref[0, 0:1]
    level = jnp.where(lane < 128, whole, shared)
    cut = jnp.zeros((1, 256), jnp.int32)
    for z in range(Z):
        cut = jnp.where(level == z, cuts[:, z : z + 1], cut)
    index = lax.broadcasted_iota(jnp.int32, (128, 1), 0)

    def kept(values, group):
        wave = 4 * index + group
        weight = jnp.where(wave == 0, 1.0 / NX, 2.0 / NX)
        return jnp.where(wave <= cut, values * weight, 0.0)

    def part(values, i):
        return values[128 * i : 128 * (i + 1)]

    re1 = kept(part(yc, 0) - part(yd, 1), 1)
    im1 = kept(part(yc, 1) + part(yd, 0), 1)
    re3 = kept(part(yc, 2) + part(yd, 3), 3)
    im3 = kept(part(yc, 3) - part(yd, 2), 3)

    coeffs = jnp.concatenate(
        [
            kept(part(x0, 0), 0),
            kept(part(x0, 1), 0),
            kept(part(x2, 0), 2),
            kept(part(x2, 1), 2),
            re1,
            im1,
            re3,
            im3,
        ],
        axis=0,
    )
    c_ref[0], c_ref[1] = halves(coeffs)
    column = t_ref[...]
    row = jnp.concatenate(
        [jnp.sum(column * coeffs[:, 128 * i : 128 * (i + 1)], axis=0, keepdims=True) for i in range(2)],
        axis=1,
    )
    p_ref[...] = jnp.broadcast_to(row, (8, 256))


def inverse_kernel(bound_ref, c_ref, fa_ref, ne_ref, o_ref, w_ref, ih_ref, il_ref):
    rows_of_places(fa_ref, ne_ref, ih_ref, il_ref)
    weights(bound_ref, w_ref)

    def back(columns, data):
        return dot3((ih_ref[:, columns], il_ref[:, columns]), data)

    def rows(i, first, last):
        return c_ref[i, 128 * first : 128 * last]

    p0 = back(slice(0, 256), (rows(0, 0, 2), rows(1, 0, 2)))
    p2 = back(slice(256, 512), (rows(0, 2, 4), rows(1, 2, 4)))
    co = back(slice(512, 1024), (rows(0, 4, 8), rows(1, 4, 8)))
    turned = [
        jnp.concatenate([rows(i, 5, 6), -rows(i, 4, 5), -rows(i, 7, 8), rows(i, 6, 7)], axis=0)
        for i in range(2)
    ]
    do = back(slice(512, 1024), turned)
    even, odd = p0 + p2, p0 - p2
    for u, value in enumerate((even + co, odd + do, even - co, odd - do)):
        owned = slice(16 * u, 16 * (u + 1))
        o_ref[owned, 0:4] = value[:, :128].reshape(16, 4, 8, 128)
        rest = value[:, 128:].reshape(16, 4, 8, 128)
        above, below = rest[:, 0:2], rest[:, 2:4]
        o_ref[owned, 4:6] = jnp.where(half_lanes(above), above, swapped(below))


def blend_kernel(s_ref, w_ref, p_ref, o_ref):
    whole = p_ref[0:1, :128]
    shared = p_ref[0:1, 128:]
    shared = jnp.where(half_lanes(shared), shared, swapped(shared))
    for tiles, inflow in ((slice(0, 4), whole), (slice(4, 6), shared)):
        smooth = s_ref[:, tiles]
        o_ref[:, tiles] = smooth + w_ref[:, tiles] * (inflow[None, None] - smooth)


def synthesis_kernel(q_ref, table_ref, o_hbm, o_ref, sems):
    copies = []
    for i, (begin, end) in enumerate(CHUNKS):
        sums = []
        for parity in range(2):
            rows = []
            for f in range(begin, end):
                blocks = []
                for part in range(2):
                    block = 4 * f + 2 * parity + part
                    first = block // 3 * 2
                    if block % 3 != 1:
                        blocks.append(q_ref[first + block % 3 // 2, 0:4].reshape(ROWS, 128))
                        continue
                    even = q_ref[first, 4:6].reshape(16, 128)
                    odd = q_ref[first + 1, 4:6].reshape(16, 128)
                    low = half_lanes(even)
                    above = jnp.where(low, even, swapped(odd))
                    below = jnp.where(low, swapped(even), odd)
                    blocks.append(jnp.concatenate([above, below], axis=0))
                rows.append(jnp.concatenate(blocks, axis=1))
            data = halves(jnp.concatenate(rows, axis=0))
            sums.append(dot3(data, (table_ref[parity, 0], table_ref[parity, 1])))
        dims = (end - begin, ROWS, NY // 2)
        o_ref[begin:end, :, : NY // 2] = (sums[0] + sums[1]).reshape(dims)
        o_ref[begin:end, :, NY // 2 :] = (sums[0] - sums[1]).reshape(dims)
        fields = pl.ds(begin, end - begin)
        copies.append(
            pltpu.make_async_copy(o_ref.at[fields], o_hbm.at[fields], sems.at[i])
        )
        copies[-1].start()
    for copy in copies:
        copy.wait()


def whole(space):
    return pl.BlockSpec(memory_space=space)


def params(mib):
    return pltpu.CompilerParams(vmem_limit_bytes=mib * 1024 * 1024)


def shape(*dims, kind=F32):
    return jax.ShapeDtypeStruct(dims, kind)


PIECES = shape(DEVICES, *PIECE)
FIELDS = (COMP * Z, ROWS, NY)


def on_device(velocity, cutoffs, plane_index, boundary_index):
    spectra = pl.pallas_call(
        analysis_kernel,
        in_specs=[whole(HBM)] * 3,
        out_specs=whole(HBM),
        out_shape=PIECES,
        scratch_shapes=[
            pltpu.VMEM(PIECES.shape, F32),
            pltpu.VMEM(FIELDS, F32),
            pltpu.SMEM((1, 2, Z), jnp.int32),
            pltpu.VMEM((2, 2, 48, 128), F32),
            pltpu.VMEM((2, 2, NY // 2, KY), BF16),
            pltpu.SemaphoreType.DMA((2 + 2 * len(CHUNKS),)),
        ],
        compiler_params=params(63),
        name="analysis",
    )(velocity.reshape(FIELDS), cutoffs, jnp.asarray(parts_y()))
    columns = lax.all_to_all(spectra, SLAB, 0, 0, tiled=True)
    coarse, fine, far, near = (jnp.asarray(part) for part in angle_parts())
    coeffs, plane = pl.pallas_call(
        forward_kernel,
        in_specs=[whole(VMEM), whole(SMEM)] + [whole(VMEM)] * 3,
        out_specs=[whole(VMEM)] * 2,
        out_shape=[shape(2, 2 * KX, 256, kind=BF16), shape(8, 256)],
        scratch_shapes=[pltpu.VMEM((2 * KX, QUARTER), BF16)] * 2 + [pltpu.VMEM((2 * KX, 128), F32)],
        compiler_params=params(24),
        name="forward",
    )(cutoffs, plane_index, columns, coarse, fine)
    members = lax.axis_size("ens")
    route = [((i - 1) % members, i) for i in range(members)]
    inflow = lax.ppermute(plane, "ens", route)
    smooth, weight = pl.pallas_call(
        inverse_kernel,
        in_specs=[whole(SMEM)] + [whole(VMEM)] * 3,
        out_specs=[whole(VMEM)] * 2,
        out_shape=[PIECES] * 2,
        scratch_shapes=[pltpu.VMEM((QUARTER, 2 * KX), BF16)] * 2,
        compiler_params=params(24),
        cost_estimate=pl.CostEstimate(flops=1 << 30, bytes_accessed=1 << 22, transcendentals=0),
        name="inverse",
    )(boundary_index, coeffs, far, near)
    blended = pl.pallas_call(
        blend_kernel,
        in_specs=[whole(VMEM)] * 3,
        out_specs=whole(VMEM),
        out_shape=PIECES,
        compiler_params=params(8),
        name="blend",
    )(smooth, weight, inflow)
    returned = lax.all_to_all(blended, SLAB, 0, 0, tiled=True)
    result = pl.pallas_call(
        synthesis_kernel,
        in_specs=[whole(VMEM), whole(VMEM)],
        out_specs=whole(HBM),
        out_shape=shape(*FIELDS),
        scratch_shapes=[pltpu.VMEM(FIELDS, F32), pltpu.SemaphoreType.DMA((len(CHUNKS),))],
        compiler_params=params(24),
        name="synthesis",
    )(returned, jnp.asarray(basis_y()))
    return result.reshape(1, COMP, Z, ROWS, NY)


def solution(mesh):
    split = Mesh(
        mesh.devices.reshape(mesh.shape["ens"], 4, 8, 2), ("ens", "slab_0", "slab_1", "slab_2")
    )
    in_specs = (P("ens", None, None, SLAB, None), P("ens", None, None), P("ens"), P("ens"))
    out_specs = P("ens", None, None, SLAB, None)
    return jax.shard_map(
        on_device, mesh=split, in_specs=in_specs, out_specs=out_specs, check_vma=False
    )
```

```python
import jax
import jax.numpy as jnp
import ml_dtypes
import numpy as np
from jax import lax
from jax.experimental import pallas as pl
from jax.experimental.pallas import tpu as pltpu
from jax.sharding import Mesh
from jax.sharding import PartitionSpec as P

NX = 2048
NY = 1024
KX = 512
KY = 256
COMP = 3
Z = 8
DEVICES = 64
ROWS = NX // DEVICES
SLAB = ("slab_0", "slab_1", "slab_2")

PIECE = (6, 8, 128)
QUARTER = NX // 4
CHUNKS = ((0, 8), (8, 16), (16, 24))
CHUNKS_OUT = ((0, 4), (4, 8), (8, 12), (12, 16), (16, 20), (20, 24))
F32 = jnp.float32
BF16 = jnp.bfloat16
VMEM = pltpu.MemorySpace.VMEM
SMEM = pltpu.MemorySpace.SMEM
HBM = pltpu.MemorySpace.HBM


def halves(x):
    high = x.astype(BF16)
    return high, (x - high.astype(F32)).astype(BF16)


def dot3(left, right):
    def one(a, b):
        return jnp.dot(a, b, preferred_element_type=F32)

    (lh, ll), (rh, rl) = left, right
    return one(lh, rh) + (one(ll, rh) + one(lh, rl))


def basis_y():
    parity = np.arange(2)[:, None, None]
    row = np.arange(KY)[None, :, None]
    place = np.arange(NY // 2)[None, None, :]
    phase = (place * (2 * (row % 128) + parity)) % NY
    angle = phase * (2.0 * np.pi / NY)
    table = np.where(row < 128, np.cos(angle), np.sin(angle))
    high = table.astype(ml_dtypes.bfloat16)
    low = (table - high.astype(np.float64)).astype(ml_dtypes.bfloat16)
    return np.stack([high, low], axis=1)


def parts_y():
    wave = 2 * np.arange(128)[None, :]
    place = np.concatenate([16 * np.arange(32), np.arange(16)])[:, None]
    return np.stack([turns(wave + parity, place, NY) for parity in range(2)])


GROUPS = (0, 2, 1, 3)


def turns(left, right, length=NX):
    phase = (left * right) % length
    angle = phase * (2.0 * np.pi / length)
    return np.stack([np.cos(angle), np.sin(angle)]).astype(np.float32)


def angle_parts():
    place = np.arange(QUARTER)[None, :]
    sixteen = np.arange(16)[:, None]
    coarse = turns(64 * np.arange(8)[:, None], place)
    fine = np.stack([turns(4 * sixteen + g, place) for g in GROUPS])
    wave = 4 * np.arange(128)[None, :]
    far = np.stack([turns(wave + g, 16 * np.arange(32)[:, None]) for g in GROUPS])
    near = np.stack([turns(wave + g, sixteen) for g in GROUPS])
    return coarse, fine, far, near


def products(a, b):
    return a[0] * b[0] - a[1] * b[1], a[1] * b[0] + a[0] * b[1]


def store(high_ref, low_ref, rows, columns, value):
    high_ref[rows, columns], low_ref[rows, columns] = halves(value)


def rows_of_waves(plane_ref, ca_ref, fi_ref, fh_ref, fl_ref, t_ref):
    at = plane_ref[0]

    def picked(value):
        here = lax.broadcasted_iota(jnp.int32, value.shape, 1) == at % QUARTER
        return jnp.sum(jnp.where(here, value, 0.0), axis=1, keepdims=True)

    coarse_at = picked(ca_ref[0]), picked(ca_ref[1])
    for g in range(4):
        fine = fi_ref[g, 0], fi_ref[g, 1]
        turn = at // QUARTER * GROUPS[g] % 4
        cosine = jnp.where(turn % 2 == 0, 1 - turn, 0).astype(F32)
        sine = jnp.where(turn % 2 == 1, 2 - turn, 0).astype(F32)
        c, s = picked(fine[0]), picked(fine[1])
        fine_at = cosine * c - sine * s, sine * c + cosine * s
        for n in range(8):
            coarse = ca_ref[0, n : n + 1], ca_ref[1, n : n + 1]
            there = coarse_at[0][n : n + 1], coarse_at[1][n : n + 1]
            values, at_plane = products(coarse, fine), products(there, fine_at)
            for i in range(2):
                first = 256 * g + 128 * i + 16 * n
                rows = slice(first, first + 16)
                store(fh_ref, fl_ref, rows, slice(None), values[i])
                t_ref[rows] = jnp.broadcast_to(at_plane[i], (16, 128))


def rows_of_places(fa_ref, ne_ref, ih_ref, il_ref):
    for g in range(4):
        near = ne_ref[g, 0], ne_ref[g, 1]
        for b in range(32):
            far = fa_ref[g, 0, b : b + 1], fa_ref[g, 1, b : b + 1]
            for i, value in enumerate(products(far, near)):
                first = 256 * g + 128 * i
                store(ih_ref, il_ref, slice(16 * b, 16 * b + 16), slice(first, first + 128), value)


def weights(bound_ref, w_ref):
    def relax(place):
        offset = jnp.abs(place - bound_ref[0])
        distance = jnp.minimum(offset, NX - offset)
        return jnp.exp(-distance.astype(F32) / (NX / 4.0))

    for g in range(8):
        place = 32 * (8 * g + lax.broadcasted_iota(jnp.int32, (8, 4, 8, 128), 0))
        place += 8 * lax.broadcasted_iota(jnp.int32, place.shape, 1)
        place += lax.broadcasted_iota(jnp.int32, place.shape, 2)
        w_ref[8 * g : 8 * g + 8, 0:4] = relax(place)
        rest = place[:, 0:2]
        w_ref[8 * g : 8 * g + 8, 4:6] = relax(jnp.where(half_lanes(rest), rest, rest + 16))


def half_lanes(x):
    return lax.broadcasted_iota(jnp.int32, (1,) * (x.ndim - 1) + (128,), x.ndim - 1) < 64


def swapped(x):
    return pltpu.roll(x, 64, x.ndim - 1)


def analysis_kernel(
    v_hbm, cut_hbm, part_hbm, o_hbm, o_ref, v_ref, cut_ref, part_ref, table_ref, sems
):
    copies = [
        pltpu.make_async_copy(part_hbm, part_ref, sems.at[0]),
        pltpu.make_async_copy(cut_hbm, cut_ref, sems.at[1]),
    ]
    for i, (first, last) in enumerate(CHUNKS):
        fields = pl.ds(first, last - first)
        copies.append(
            pltpu.make_async_copy(v_hbm.at[fields], v_ref.at[fields], sems.at[2 + i])
        )
    for copy in copies:
        copy.start()
    for copy in copies[:2]:
        copy.wait()
    for parity in range(2):
        near = part_ref[parity, 0, 32:48], part_ref[parity, 1, 32:48]
        for b in range(32):
            far = part_ref[parity, 0, b : b + 1], part_ref[parity, 1, b : b + 1]
            for i, value in enumerate(products(far, near)):
                rows, columns = slice(16 * b, 16 * b + 16), slice(128 * i, 128 * i + 128)
                high, low = halves(value)
                table_ref[parity, 0, rows, columns] = high
                table_ref[parity, 1, rows, columns] = low
    lane = lax.broadcasted_iota(jnp.int32, (1, KY), 1) % 128
    sent = 0
    for i, (begin, end) in enumerate(CHUNKS):
        copies[2 + i].wait()
        field = v_ref[begin:end].reshape((end - begin) * ROWS, NY)
        left, right = field[:, : NY // 2], field[:, NY // 2 :]
        for parity in range(2):
            folded = left - right if parity else left + right
            spectra = dot3(halves(folded), (table_ref[parity, 0], table_ref[parity, 1]))
            wave = 2 * lane + parity
            weight = jnp.where(wave == 0, 1.0 / NY, 2.0 / NY)
            for f in range(begin, end):
                scale = jnp.where(wave <= cut_ref[0, 1, f % Z], weight, 0.0)
                own = spectra[ROWS * (f - begin) : ROWS * (f - begin + 1)] * scale
                for part in range(2):
                    block = 4 * f + 2 * parity + part
                    values = own[:, 128 * part : 128 * (part + 1)]
                    first = block // 3 * 2
                    if block % 3 != 1:
                        o_ref[first + block % 3 // 2, 0:4] = values.reshape(4, 8, 128)
                        continue
                    above, below = values[:16], values[16:]
                    low = half_lanes(above)
                    even = jnp.where(low, above, swapped(below))
                    odd = jnp.where(low, swapped(above), below)
                    o_ref[first, 4:6] = even.reshape(2, 8, 128)
                    o_ref[first + 1, 4:6] = odd.reshape(2, 8, 128)
        ready = pl.ds(sent, 4 * end // 3 * 2 - sent)
        sent = 4 * end // 3 * 2
        done = pltpu.make_async_copy(
            o_ref.at[ready], o_hbm.at[ready], sems.at[2 + len(CHUNKS) + i]
        )
        done.start()
        copies.append(done)
    for copy in copies[2 + len(CHUNKS) :]:
        copy.wait()


def forward_kernel(cut_ref, plane_ref, r_ref, ca_ref, fi_ref, c_ref, p_ref, fh_ref, fl_ref, t_ref):
    rows_of_waves(plane_ref, ca_ref, fi_ref, fh_ref, fl_ref, t_ref)
    quarters = []
    for u in range(4):
        owned = slice(16 * u, 16 * (u + 1))
        main = r_ref[owned, 0:4].reshape(QUARTER, 128)
        rest = r_ref[owned, 4:6]
        rest = jnp.concatenate([rest, swapped(rest)], axis=1).reshape(QUARTER, 128)
        quarters.append(jnp.concatenate([main, rest], axis=1))
    v0, v1, v2, v3 = quarters
    even, odd = v0 + v2, v1 + v3
    inputs = [halves(even + odd), halves(even - odd), halves(v0 - v2), halves(v1 - v3)]

    def ahead(rows, data):
        return dot3((fh_ref[rows], fl_ref[rows]), data)

    x0 = ahead(slice(0, 256), inputs[0])
    x2 = ahead(slice(256, 512), inputs[1])
    yc = ahead(slice(512, 1024), inputs[2])
    yd = ahead(slice(512, 1024), inputs[3])
    pair = 8 * lax.axis_index("slab_0") + lax.axis_index("slab_1")
    whole = (3 * pair + 2 * lax.axis_index("slab_2")) // 4 % Z
    shared = (3 * pair + 1) // 4 % Z
    lane = lax.broadcasted_iota(jnp.int32, (1, 256), 1)
    cuts = cut_ref[0, 0:1]
    level = jnp.where(lane < 128, whole, shared)
    cut = jnp.zeros((1, 256), jnp.int32)
    for z in range(Z):
        cut = jnp.where(level == z, cuts[:, z : z + 1], cut)
    index = lax.broadcasted_iota(jnp.int32, (128, 1), 0)

    def kept(values, group):
        wave = 4 * index + group
        weight = jnp.where(wave == 0, 1.0 / NX, 2.0 / NX)
        return jnp.where(wave <= cut, values * weight, 0.0)

    def part(values, i):
        return values[128 * i : 128 * (i + 1)]

    re1 = kept(part(yc, 0) - part(yd, 1), 1)
    im1 = kept(part(yc, 1) + part(yd, 0), 1)
    re3 = kept(part(yc, 2) + part(yd, 3), 3)
    im3 = kept(part(yc, 3) - part(yd, 2), 3)

    coeffs = jnp.concatenate(
        [
            kept(part(x0, 0), 0),
            kept(part(x0, 1), 0),
            kept(part(x2, 0), 2),
            kept(part(x2, 1), 2),
            re1,
            im1,
            re3,
            im3,
        ],
        axis=0,
    )
    c_ref[...] = coeffs
    column = t_ref[...]
    row = jnp.concatenate(
        [jnp.sum(column * coeffs[:, 128 * i : 128 * (i + 1)], axis=0, keepdims=True) for i in range(2)],
        axis=1,
    )
    p_ref[...] = jnp.broadcast_to(row, (8, 256))


def inverse_kernel(bound_ref, c_ref, fa_ref, ne_ref, o_ref, w_ref, ih_ref, il_ref):
    rows_of_places(fa_ref, ne_ref, ih_ref, il_ref)
    weights(bound_ref, w_ref)

    def back(columns, data):
        return dot3((ih_ref[:, columns], il_ref[:, columns]), data)

    split = halves(c_ref[...])

    def rows(i, first, last):
        return split[i][128 * first : 128 * last]

    p0 = back(slice(0, 256), (rows(0, 0, 2), rows(1, 0, 2)))
    p2 = back(slice(256, 512), (rows(0, 2, 4), rows(1, 2, 4)))
    co = back(slice(512, 1024), (rows(0, 4, 8), rows(1, 4, 8)))
    turned = [
        jnp.concatenate([rows(i, 5, 6), -rows(i, 4, 5), -rows(i, 7, 8), rows(i, 6, 7)], axis=0)
        for i in range(2)
    ]
    do = back(slice(512, 1024), turned)
    even, odd = p0 + p2, p0 - p2
    for u, value in enumerate((even + co, odd + do, even - co, odd - do)):
        owned = slice(16 * u, 16 * (u + 1))
        o_ref[owned, 0:4] = value[:, :128].reshape(16, 4, 8, 128)
        rest = value[:, 128:].reshape(16, 4, 8, 128)
        above, below = rest[:, 0:2], rest[:, 2:4]
        o_ref[owned, 4:6] = jnp.where(half_lanes(above), above, swapped(below))


def blend_kernel(s_ref, w_ref, p_ref, o_ref):
    whole = p_ref[0:1, :128]
    shared = p_ref[0:1, 128:]
    shared = jnp.where(half_lanes(shared), shared, swapped(shared))
    for tiles, inflow in ((slice(0, 4), whole), (slice(4, 6), shared)):
        smooth = s_ref[:, tiles]
        o_ref[:, tiles] = smooth + w_ref[:, tiles] * (inflow[None, None] - smooth)


def synthesis_kernel(q_ref, table_ref, o_hbm, o_ref, sems):
    copies = []
    for i, (begin, end) in enumerate(CHUNKS_OUT):
        sums = []
        for parity in range(2):
            rows = []
            for f in range(begin, end):
                blocks = []
                for part in range(2):
                    block = 4 * f + 2 * parity + part
                    first = block // 3 * 2
                    if block % 3 != 1:
                        blocks.append(q_ref[first + block % 3 // 2, 0:4].reshape(ROWS, 128))
                        continue
                    even = q_ref[first, 4:6].reshape(16, 128)
                    odd = q_ref[first + 1, 4:6].reshape(16, 128)
                    low = half_lanes(even)
                    above = jnp.where(low, even, swapped(odd))
                    below = jnp.where(low, swapped(even), odd)
                    blocks.append(jnp.concatenate([above, below], axis=0))
                rows.append(jnp.concatenate(blocks, axis=1))
            data = halves(jnp.concatenate(rows, axis=0))
            sums.append(dot3(data, (table_ref[parity, 0], table_ref[parity, 1])))
        dims = (end - begin, ROWS, NY // 2)
        o_ref[begin:end, :, : NY // 2] = (sums[0] + sums[1]).reshape(dims)
        o_ref[begin:end, :, NY // 2 :] = (sums[0] - sums[1]).reshape(dims)
        fields = pl.ds(begin, end - begin)
        copies.append(
            pltpu.make_async_copy(o_ref.at[fields], o_hbm.at[fields], sems.at[i])
        )
        copies[-1].start()
    for copy in copies:
        copy.wait()


def whole(space):
    return pl.BlockSpec(memory_space=space)


def params(mib):
    return pltpu.CompilerParams(vmem_limit_bytes=mib * 1024 * 1024)


def shape(*dims, kind=F32):
    return jax.ShapeDtypeStruct(dims, kind)


PIECES = shape(DEVICES, *PIECE)
FIELDS = (COMP * Z, ROWS, NY)


def on_device(velocity, cutoffs, plane_index, boundary_index):
    spectra = pl.pallas_call(
        analysis_kernel,
        in_specs=[whole(HBM)] * 3,
        out_specs=whole(HBM),
        out_shape=PIECES,
        scratch_shapes=[
            pltpu.VMEM(PIECES.shape, F32),
            pltpu.VMEM(FIELDS, F32),
            pltpu.SMEM((1, 2, Z), jnp.int32),
            pltpu.VMEM((2, 2, 48, 128), F32),
            pltpu.VMEM((2, 2, NY // 2, KY), BF16),
            pltpu.SemaphoreType.DMA((2 + 2 * len(CHUNKS),)),
        ],
        compiler_params=params(63),
        name="analysis",
    )(velocity.reshape(FIELDS), cutoffs, jnp.asarray(parts_y()))
    columns = lax.all_to_all(spectra, SLAB, 0, 0, tiled=True)
    coarse, fine, far, near = (jnp.asarray(part) for part in angle_parts())
    coeffs, plane = pl.pallas_call(
        forward_kernel,
        in_specs=[whole(VMEM), whole(SMEM)] + [whole(VMEM)] * 3,
        out_specs=[whole(VMEM)] * 2,
        out_shape=[shape(2 * KX, 256), shape(8, 256)],
        scratch_shapes=[pltpu.VMEM((2 * KX, QUARTER), BF16)] * 2 + [pltpu.VMEM((2 * KX, 128), F32)],
        compiler_params=params(24),
        name="forward",
    )(cutoffs, plane_index, columns, coarse, fine)
    members = lax.axis_size("ens")
    route = [((i - 1) % members, i) for i in range(members)]
    inflow = lax.ppermute(plane, "ens", route)
    smooth, weight = pl.pallas_call(
        inverse_kernel,
        in_specs=[whole(SMEM)] + [whole(VMEM)] * 3,
        out_specs=[whole(VMEM)] * 2,
        out_shape=[PIECES] * 2,
        scratch_shapes=[pltpu.VMEM((QUARTER, 2 * KX), BF16)] * 2,
        compiler_params=params(24),
        cost_estimate=pl.CostEstimate(flops=1 << 30, bytes_accessed=1 << 22, transcendentals=0),
        name="inverse",
    )(boundary_index, coeffs, far, near)
    blended = pl.pallas_call(
        blend_kernel,
        in_specs=[whole(VMEM)] * 3,
        out_specs=whole(VMEM),
        out_shape=PIECES,
        compiler_params=params(8),
        name="blend",
    )(smooth, weight, inflow)
    returned = lax.all_to_all(blended, SLAB, 0, 0, tiled=True)
    result = pl.pallas_call(
        synthesis_kernel,
        in_specs=[whole(VMEM), whole(VMEM)],
        out_specs=whole(HBM),
        out_shape=shape(*FIELDS),
        scratch_shapes=[pltpu.VMEM(FIELDS, F32), pltpu.SemaphoreType.DMA((len(CHUNKS_OUT),))],
        compiler_params=params(24),
        name="synthesis",
    )(returned, jnp.asarray(basis_y()))
    return result.reshape(1, COMP, Z, ROWS, NY)


def solution(mesh):
    split = Mesh(
        mesh.devices.reshape(mesh.shape["ens"], 4, 8, 2), ("ens", "slab_0", "slab_1", "slab_2")
    )
    in_specs = (P("ens", None, None, SLAB, None), P("ens", None, None), P("ens"), P("ens"))
    out_specs = P("ens", None, None, SLAB, None)
    return jax.shard_map(
        on_device, mesh=split, in_specs=in_specs, out_specs=out_specs, check_vma=False
    )
```
